256 devices in a mesh: ep: 128 (over z, x, y), half: 2 (over core).
Axes of the slice: x: 4, y: 4, z: 8, core: 2. Of those that a mesh axis runs over, the one named last changes fastest.
Arguments:
- tokens: bfloat16 [16384, 2048], P('ep', 'half'), may hold values from -6 to 6
- gate_weights: float32 [16384, 8], P('ep'), may hold values from 0.05 to 0.3
- expert_ids: int32 [16384, 8], P('ep'), may hold values from 0 to 127, all different within a row; in each aligned block of 128 rows (0 to 127, 128 to 255, ...) at most 10 rows name the same one
- w_gate: bfloat16 [128, 2048, 768], P('ep', None, 'half'), may hold values from -0.125 to 0.125
- w_up: bfloat16 [128, 2048, 768], P('ep', None, 'half'), may hold values from -0.125 to 0.125
- w_down: bfloat16 [128, 768, 2048], P('ep', 'half'), may hold values from -0.21875 to 0.21875
Outputs:
- mixed: bfloat16 [16384, 2048], P('ep', 'half')
The draws below stay inside these ranges and needn't reach their ends.
Inputs may be any that keep to these rules, and one draw needn't show every extreme that they name: `expert_ids`: each row names 8 different experts. Within the rows of one device (aligned blocks of 128 rows) no expert is named by more than 10 rows, and in every draw some expert is named by exactly 10 rows of some block.
All inputs are finite; a program needn't handle non-finite values.
Results may differ from the reference program's by a relative error of at most 0.0085.
Values may be sent and summed in bfloat16 or wider, within the bound.
No kernel may reach another device: no remote copies, remote signals or barrier semaphores. Data moves between devices by JAX's collectives and lax.ppermute only.
A program may use at most 64 MiB of HBM per device.

```python
import math
import jax
import jax.numpy as jnp
import numpy as np
from jax import lax

D = 2048
FF = 768
TOP = 8
TOK_DEV = 128
EXPERTS = 128
TOKENS = 16384
CAP = 10
N_EP = 128


def steps_of(own_key, shape, shards, low, largest):
    factor_of = 1.0
    for axis_at, shards_of in shards:
        steps = jax.random.uniform(jax.random.fold_in(jax.random.fold_in(own_key, 6), axis_at), (shards_of,), jnp.float32, low / len(shards), largest / len(shards))
        factor_of = factor_of * jnp.repeat(jnp.exp(steps), shape[axis_at] // shards_of).reshape((-1,) + (1,) * (len(shape) - 1 - axis_at))
    return factor_of


def deal_out(rng, own, number, rows, amount, top, reach, slope):
    sequence = jax.random.permutation(rng, amount)
    crowded, common = shares(amount, rows * top, reach, slope, True), shares(amount, rows * top, reach, slope, False)
    places = jnp.arange(amount)

    def named(lengths, rotation):
        used = int((lengths > 0).sum())
        fixed = max(1, used // 4)
        passed = fixed + (places - fixed + rotation * (used - fixed)) % max(1, amount - fixed)
        return jnp.zeros((amount,), jnp.int32).at[sequence[jnp.where(places < fixed, places, passed)]].set(jnp.asarray(lengths, jnp.int32))

    lengths = jnp.where(number % 4 == 0, named(crowded, number // 4), named(common, number - number // 4 - 1))
    mixed = jax.random.permutation(jax.random.fold_in(own, 3), amount)
    giver, receiver = mixed[0:amount // 2 * 2:2], mixed[1:amount // 2 * 2:2]
    margin = jnp.minimum(lengths[giver] - 1, reach - lengths[receiver]) // 2
    margin = jnp.where((giver == sequence[0]) | (receiver == sequence[0]) | (lengths[receiver] == 0), 0, jnp.maximum(margin, 0))
    passed = jax.random.randint(jax.random.fold_in(own, 4), (amount // 2,), 0, 1 << 20) % (margin + 1)
    lengths = lengths.at[giver].add(-passed).at[receiver].add(passed)
    items = jnp.searchsorted(jnp.cumsum(lengths), jnp.arange(rows * top), side="right").astype(jnp.int32)
    table = items.reshape(top, rows).T
    table = table[jax.random.permutation(jax.random.fold_in(own, 1), rows)]
    rotation = jax.random.randint(jax.random.fold_in(own, 2), (rows, 1), 0, top)
    return jnp.take_along_axis(table, (jnp.arange(top)[None, :] + rotation) % top, axis=1)


def shares(amount, total, limit, lean, full):
    weights = [(1 << 20) // math.isqrt(rank ** lean) + 1 for rank in range(1, amount + 1)]
    largest = limit if full else min(limit, max(-(-total // amount), total * weights[0] // sum(weights)))
    least = 1 if total - largest >= amount - 1 else 0
    holding, rest = [largest] + [least] * (amount - 1), total - largest - least * (amount - 1)
    while rest > 0:
        candidates = [i for i in range(1, amount) if holding[i] < largest] or [i for i in range(1, amount) if holding[i] < limit]
        pool, remaining = sum([weights[i] for i in candidates]), rest
        for i in candidates:
            more = min(limit - holding[i], max(1, remaining * weights[i] // pool), rest)
            holding[i] = holding[i] + more
            rest = rest - more
    return np.array(holding)


def scatter_about(key, extent, deviation, reach, shards=(), kind=jnp.bfloat16):
    entries = jax.random.normal(key, extent, jnp.float32) * deviation
    if len(shards) > 0:
        entries = steps_of(key, extent, shards, -0.22, 0.18) * entries
    return jnp.clip(entries, min=-reach, max=reach).astype(kind)


def setup_inputs(seed: int = 0) -> dict:
    arg_keys = jax.random.split(jax.random.key(seed), 7)
    tokens = scatter_about(arg_keys[0], (TOKENS, D), 1.0, 6.0, ((0, 128), (1, 2)))
    gate_weights = jnp.clip(0.05 + 0.25 * jax.random.uniform(arg_keys[1], (TOKENS, TOP), jnp.float32) ** steps_of(arg_keys[1], (TOKENS, TOP), ((0, 128),), -0.2, 0.2), 0.05, 0.3)
    expert_ids_keys = jax.random.split(jax.random.fold_in(arg_keys[2], 1), TOKENS // TOK_DEV)
    expert_ids_turns = jax.random.permutation(jax.random.fold_in(arg_keys[2], 3), TOKENS // TOK_DEV)
    expert_ids = jax.vmap(lambda own, number: deal_out(jax.random.fold_in(arg_keys[2], 2), own, number, TOK_DEV, EXPERTS, TOP, CAP, 2))(expert_ids_keys, expert_ids_turns).reshape((TOKENS, TOP))
    w_gate = scatter_about(arg_keys[3], (EXPERTS, D, FF), D ** -0.5, 0.125, ((0, 128), (2, 2)))
    w_up = scatter_about(arg_keys[4], (EXPERTS, D, FF), D ** -0.5, 0.125, ((0, 128), (2, 2)))
    w_down = scatter_about(arg_keys[5], (EXPERTS, FF, D), FF ** -0.5, 0.21875, ((0, 128), (1, 2)))
    return {"tokens": tokens, "gate_weights": gate_weights, "expert_ids": expert_ids, "w_gate": w_gate, "w_up": w_up, "w_down": w_down}


def rank_block(block):
    columns = jnp.arange(EXPERTS, dtype=jnp.int32)
    onehot = (block[:, None] == columns[None, :]).astype(jnp.int32)
    before = jnp.cumsum(onehot, axis=0) - onehot
    return jnp.sum(before * onehot, axis=1).astype(jnp.int32)


def reference(tokens, gate_weights, expert_ids, w_gate, w_up, w_down):
    ids = expert_ids.reshape(N_EP, TOK_DEV * TOP).astype(jnp.int32)
    ranks = lax.map(rank_block, ids)
    slot = (ids * CAP + ranks).astype(jnp.int32)
    source = jnp.arange(N_EP, dtype=jnp.int32)[:, None]
    local_token = (jnp.arange(TOK_DEV * TOP, dtype=jnp.int32) // TOP)[None, :]
    token_table = jnp.zeros((N_EP, EXPERTS * CAP), jnp.int32).at[source, slot].set(source * TOK_DEV + local_token)
    weight_table = jnp.zeros((N_EP, EXPERTS * CAP), jnp.float32).at[source, slot].set(gate_weights.reshape(N_EP, TOK_DEV * TOP))
    filled = jnp.zeros((N_EP, EXPERTS * CAP), jnp.bfloat16).at[source, slot].set(jnp.ones((N_EP, TOK_DEV * TOP), jnp.bfloat16))
    token_table = token_table.reshape(N_EP, EXPERTS, CAP).transpose(1, 0, 2).reshape(EXPERTS, N_EP * CAP)
    weight_table = weight_table.reshape(N_EP, EXPERTS, CAP).transpose(1, 0, 2).reshape(EXPERTS, N_EP * CAP)
    filled = filled.reshape(N_EP, EXPERTS, CAP).transpose(1, 0, 2).reshape(EXPERTS, N_EP * CAP)
    middle = FF // 2

    def expert_step(total, inputs):
        gate_mat, up_mat, down_mat, rows, weights, used = inputs
        slot_rows = tokens[rows] * used[:, None]
        gate = jnp.dot(slot_rows, gate_mat, preferred_element_type=jnp.float32)
        up = jnp.dot(slot_rows, up_mat, preferred_element_type=jnp.float32)
        hidden = (jax.nn.silu(gate) * up).astype(jnp.bfloat16)
        first = jnp.dot(hidden[:, :middle], down_mat[:middle], preferred_element_type=jnp.float32)
        second = jnp.dot(hidden[:, middle:], down_mat[middle:], preferred_element_type=jnp.float32)
        first = lax.optimization_barrier(first.astype(jnp.bfloat16)).astype(jnp.float32)
        second = lax.optimization_barrier(second.astype(jnp.bfloat16)).astype(jnp.float32)
        expert_out = lax.optimization_barrier((first + second).astype(jnp.bfloat16)).astype(jnp.float32)
        total = total.at[rows].add(weights[:, None] * expert_out)
        return total, None

    start = jnp.zeros((TOKENS, D), jnp.float32)
    total, unused = lax.scan(expert_step, start, (w_gate, w_up, w_down, token_table, weight_table, filled))
    return total.astype(jnp.bfloat16)
```

```python
import functools

import jax
import jax.numpy as jnp
from jax import lax
from jax.experimental import pallas as pl
from jax.experimental.pallas import tpu as pltpu
from jax.sharding import Mesh, PartitionSpec as P


F32 = jnp.float32
BF16 = jnp.bfloat16
CAP = 10
TOK = 128
HW = 1024
PLANE = 16
ROWS = 40
PIECES = {0: 5, 1: 10, 2: 10, 3: 10, 4: 5}
CHUNKS = ((1, 2, 3, 0, 4),)


def lanes_of(slots):
    return slots * 2 * HW // ROWS


def iota(shape, dim):
    return lax.broadcasted_iota(jnp.int32, shape, dim)


def route_body(tok_ref, ids_ref, w_ref, out_ref):
    ids = ids_ref[...]
    experts = iota((128, TOK), 0)
    named = jnp.zeros((128, TOK), F32)
    for k in range(8):
        named = jnp.where(ids[k : k + 1, :] == experts, 1.0, named)
    before = jnp.where(iota((TOK, TOK), 0) < iota((TOK, TOK), 1), 1.0, 0.0)
    count = jnp.dot(named.astype(BF16), before.astype(BF16), preferred_element_type=F32)
    ranks = [
        jnp.sum(jnp.where(ids[k : k + 1, :] == experts, count, 0.0), axis=0, keepdims=True)
        for k in range(8)
    ]
    rank = jnp.concatenate(ranks, axis=0)
    w = w_ref[...]
    hi = w.astype(BF16)
    lo = (w - hi.astype(F32)).astype(BF16)
    out_ref[0:TOK, :] = tok_ref[...]
    out_ref[TOK : TOK + 8, 0:128] = ids.astype(F32).astype(BF16)
    out_ref[TOK : TOK + 8, 128:256] = rank.astype(BF16)
    out_ref[TOK : TOK + 8, 256:384] = hi
    out_ref[TOK : TOK + 8, 384:512] = lo
    out_ref[TOK : TOK + 8, 512:1024] = jnp.zeros((8, 512), BF16)


def slot_table(info, first, half, slots, values):
    ids = info[:, 0:128].astype(F32)
    rank = info[:, 128:256].astype(F32)
    mine = iota((PLANE, TOK), 0).astype(F32) + first.astype(F32)
    slot = jnp.full((PLANE, TOK), -1000.0, F32)
    picked = [jnp.zeros((PLANE, TOK), F32) for _ in values]
    for k in range(8):
        hit = ids[k : k + 1, :] == mine
        slot = jnp.where(hit, rank[k : k + 1, :], slot)
        for i, at in enumerate(values):
            value = info[:, at : at + 128].astype(F32)
            picked[i] = jnp.where(hit, value[k : k + 1, :], picked[i])
    slot = slot.astype(jnp.int32)
    if slots < CAP:
        slot = slot - half * slots
        slot = jnp.where((slot >= 0) & (slot < slots), slot, -1000)
    return slot, picked


def placed(slot, slots, q, value=None):
    rows = iota((PLANE, ROWS, TOK), 1)
    hit = slot[:, None, :] + q * slots == rows
    if value is None:
        out = jnp.where(hit, 1.0, 0.0)
    else:
        out = jnp.where(hit, value[:, None, :], 0.0)
    return out.astype(BF16).reshape(PLANE * ROWS, TOK)


def dispatch_body(pieces, scal_ref, *refs):
    out_ref = refs[-1]
    at = 0
    for i, d in enumerate(pieces):
        a_ref, b_ref = refs[2 * i], refs[2 * i + 1]
        slots = PIECES[d]
        lanes = lanes_of(slots)
        parts = 2 * HW // lanes
        slot, _ = slot_table(a_ref[TOK : TOK + 8, 0:512], scal_ref[0], scal_ref[1], slots, ())
        onehot = jnp.concatenate([placed(slot, slots, q) for q in range(parts)], axis=1)
        per = HW // lanes
        rows = jnp.concatenate(
            [
                (a_ref if q < per else b_ref)[0:TOK, (q % per) * lanes : (q % per + 1) * lanes]
                for q in range(parts)
            ],
            axis=0,
        )
        out_ref[:, at : at + lanes] = jnp.dot(onehot, rows, preferred_element_type=F32).astype(BF16)
        at += lanes


def expert_body(pieces, scal_ref, x_ref, gm_ref, gp_ref, um_ref, up_ref, dm_ref, dp_ref, out_ref):
    half = scal_ref[1]
    blocks = []
    at = 0
    for d in pieces:
        slots = PIECES[d]
        lanes = lanes_of(slots)
        parts = 2 * HW // lanes
        rows = x_ref[:, at : at + lanes]
        number = PLANE * slots
        index = iota((number, 1), 0)
        source = (index * (65536 // slots + 1)) >> 16
        start = source * ROWS + (index - source * slots)
        columns = iota((number, PLANE * ROWS), 1)
        blocks.append(
            jnp.concatenate(
                [
                    jnp.dot(
                        jnp.where(columns == start + q * slots, 1.0, 0.0).astype(BF16),
                        rows,
                        preferred_element_type=F32,
                    ).astype(BF16)
                    for q in range(parts)
                ],
                axis=1,
            )
        )
        at += lanes
    x = jnp.concatenate(blocks, axis=0) if len(blocks) > 1 else blocks[0]
    near = pl.multiple_of(half * HW, HW)
    far = pl.multiple_of((1 - half) * HW, HW)
    hidden = []
    for g_ref, u_ref in ((gm_ref, um_ref), (gp_ref, up_ref)):
        gate = jnp.dot(x[:, :HW], g_ref[pl.ds(near, HW), :], preferred_element_type=F32)
        gate = gate + jnp.dot(x[:, HW:], g_ref[pl.ds(far, HW), :], preferred_element_type=F32)
        up = jnp.dot(x[:, :HW], u_ref[pl.ds(near, HW), :], preferred_element_type=F32)
        up = up + jnp.dot(x[:, HW:], u_ref[pl.ds(far, HW), :], preferred_element_type=F32)
        hidden.append((gate / (1.0 + jnp.exp(-gate)) * up).astype(BF16))
    sides = []
    for side in (near, far):
        y = jnp.dot(hidden[0], dm_ref[:, pl.ds(side, HW)], preferred_element_type=F32)
        y = y + jnp.dot(hidden[1], dp_ref[:, pl.ds(side, HW)], preferred_element_type=F32)
        sides.append(y.astype(BF16))
    y = jnp.concatenate(sides, axis=1)
    at = 0
    first = 0
    for d in pieces:
        slots = PIECES[d]
        lanes = lanes_of(slots)
        parts = 2 * HW // lanes
        number = PLANE * slots
        index = iota((1, number), 1)
        source = (index * (65536 // slots + 1)) >> 16
        start = source * ROWS + (index - source * slots)
        columns = iota((PLANE * ROWS, number), 0)
        total = None
        for q in range(parts):
            spread = jnp.where(columns == start + q * slots, 1.0, 0.0).astype(BF16)
            part = jnp.dot(
                spread,
                y[first : first + number, q * lanes : (q + 1) * lanes],
                preferred_element_type=F32,
            )
            total = part if total is None else total + part
        out_ref[:, at : at + lanes] = total.astype(BF16)
        at += lanes
        first += number


def combine_body(d, has_received, last, scal_ref, y_ref, info_ref, *refs):
    slots = PIECES[d]
    lanes = lanes_of(slots)
    parts = 2 * HW // lanes
    slot, (hi, lo) = slot_table(info_ref[0:8, 0:512], scal_ref[0], scal_ref[1], slots, (256, 384))
    y = y_ref[...]
    total = None
    for value in (hi, lo):
        weights = jnp.concatenate([placed(slot, slots, q, value) for q in range(parts)], axis=1)
        part = lax.dot_general(weights, y, (((0,), (0,)), ((), ())), preferred_element_type=F32)
        total = part if total is None else total + part
    per = HW // lanes
    for side in range(2):
        value = jnp.concatenate(
            [total[(side * per + q) * TOK : (side * per + q + 1) * TOK, :] for q in range(per)], axis=1
        )
        if has_received:
            value = value + refs[side][...].astype(F32)
        out = refs[(2 if has_received else 0) + side]
        out[...] = value.astype(out.dtype)


def params():
    return pltpu.CompilerParams(vmem_limit_bytes=48 * 1024 * 1024)


def whole(shape):
    return pl.BlockSpec(shape, lambda i: (0,) * len(shape))


SMEM = pl.BlockSpec(memory_space=pltpu.SMEM)


def local(tokens, gate_weights, expert_ids, w_gate, w_up, w_down):
    z = lax.axis_index("z")
    half = lax.axis_index("half")
    zs = lax.axis_size("z")
    scal = jnp.stack([z * PLANE, half]).astype(jnp.int32)
    swap = [(0, 1), (1, 0)]
    forth = []
    for i in range(zs):
        forth.append((i * 2, (i + 1) % zs * 2))
        forth.append((i * 2 + 1, (i - 1) % zs * 2 + 1))
    back = [(b, a) for a, b in forth]

    route = pl.pallas_call(
        route_body,
        out_shape=jax.ShapeDtypeStruct((TOK + 8, HW), BF16),
        compiler_params=params(),
        name="route",
    )
    with jax.named_scope("exchange"):
        other = lax.ppermute(tokens, "half", swap)
    a = [route(tokens, expert_ids.T, gate_weights.T)]
    b = [other]
    mine = (w_gate[0], w_up[0], w_down[0])
    held = lax.optimization_barrier((other,) + mine)
    theirs = [lax.ppermute(w, "half", swap) for w in held[1:]]
    for d in range(4):
        a.append(lax.ppermute(a[-1], ("z", "half"), forth))
        b.append(lax.ppermute(b[-1], ("z", "half"), forth))

    answers = {}
    for chunk in CHUNKS:
        width = sum(lanes_of(PIECES[d]) for d in chunk)
        size = PLANE * ROWS
        arrays = []
        for d in chunk:
            arrays += [a[d], b[d]]
        sent = pl.pallas_call(
            functools.partial(dispatch_body, chunk),
            out_shape=jax.ShapeDtypeStruct((size, width), BF16),
            grid=(1,),
            in_specs=[SMEM] + [whole(v.shape) for v in arrays],
            out_specs=whole((size, width)),
            compiler_params=params(),
            name="dispatch",
        )(scal, *arrays)
        got = lax.all_to_all(sent.reshape(PLANE, ROWS, width), ("x", "y"), 0, 0, tiled=True)
        operands = (got.reshape(size, width), mine[0], theirs[0], mine[1], theirs[1], mine[2], theirs[2])
        result = pl.pallas_call(
            functools.partial(expert_body, chunk),
            out_shape=jax.ShapeDtypeStruct((size, width), BF16),
            grid=(1,),
            in_specs=[SMEM] + [whole(v.shape) for v in operands],
            out_specs=whole((size, width)),
            compiler_params=params(),
            name="expert",
        )(scal, *operands)
        back_rows = lax.all_to_all(result.reshape(PLANE, ROWS, width), ("x", "y"), 0, 0, tiled=True)
        back_rows = back_rows.reshape(size, width)
        at = 0
        for d in chunk:
            answers[d] = (back_rows, at)
            at += lanes_of(PIECES[d])

    received = ()
    for d in (4, 3, 2, 1, 0):
        value, at = answers[d]
        lanes = lanes_of(PIECES[d])
        last = d == 0
        kinds = (F32, BF16) if last else (BF16, BF16)
        outs = pl.pallas_call(
            functools.partial(combine_body, d, len(received) > 0, last),
            out_shape=[jax.ShapeDtypeStruct((TOK, HW), kind) for kind in kinds],
            grid=(1,),
            in_specs=[
                SMEM,
                pl.BlockSpec((PLANE * ROWS, lanes), functools.partial(lambda c, i: (0, c), at // lanes)),
                pl.BlockSpec((8, 512), lambda i: (TOK // 8, 0)),
            ]
            + [whole((TOK, HW)) for _ in received],
            out_specs=[whole((TOK, HW)), whole((TOK, HW))],
            compiler_params=params(),
            name="combine",
        )(scal, value, a[d], *received)
        if not last:
            received = tuple(lax.ppermute(v, ("z", "half"), back) for v in outs)
    kept, given = outs
    return (kept + lax.ppermute(given, "half", swap).astype(F32)).astype(BF16)


def solution(mesh):
    spaced = Mesh(mesh.devices.reshape(8, 4, 4, 2), ("z", "x", "y", "half"))
    ep = ("z", "x", "y")
    specs = (
        P(ep, "half"),
        P(ep, None),
        P(ep, None),
        P(ep, None, "half"),
        P(ep, None, "half"),
        P(ep, "half", None),
    )
    return jax.shard_map(
        local, mesh=spaced, in_specs=specs, out_specs=P(ep, "half"), check_vma=False
    )
```

```python
import functools

import jax
import jax.numpy as jnp
from jax import lax
from jax.experimental import pallas as pl
from jax.experimental.pallas import tpu as pltpu
from jax.sharding import Mesh, PartitionSpec as P


F32 = jnp.float32
BF16 = jnp.bfloat16
CAP = 10
TOK = 128
WIDE = 2048
PART = 512
FH = 384
PLANE = 16
SUB = 8
LEFT = WIDE // SUB
PIECES = {0: 5, 1: 10, 2: 10, 3: 10, 4: 5}
CHUNKS = ((0, 1), (2, 3, 4))


def iota(shape, dim):
    return lax.broadcasted_iota(jnp.int32, shape, dim)


def plan(chunk):
    first = {}
    n = 0
    for d in chunk:
        first[d] = n
        n += PIECES[d]
    left = n % SUB == 1
    tiles = n // SUB if left else -(-n // SUB)
    return tiles, left, first


def lanes_of(chunk):
    tiles, left, _ = plan(chunk)
    return tiles * WIDE + (LEFT if left else 0)


def tiles_of(chunk, d):
    tiles, left, first = plan(chunk)
    at, end = first[d], first[d] + PIECES[d]
    return [j for j in range(tiles) if at < (j + 1) * SUB and end > j * SUB], left and end > tiles * SUB


def route_body(tok_ref, ids_ref, w_ref, a_ref, b_ref):
    ids = ids_ref[...]
    experts = iota((128, TOK), 0)
    named = jnp.zeros((128, TOK), F32)
    for k in range(8):
        named = jnp.where(ids[k : k + 1, :] == experts, 1.0, named)
    before = jnp.where(iota((TOK, TOK), 0) < iota((TOK, TOK), 1), 1.0, 0.0)
    count = jnp.dot(named.astype(BF16), before.astype(BF16), preferred_element_type=F32)
    ranks = [
        jnp.sum(jnp.where(ids[k : k + 1, :] == experts, count, 0.0), axis=0, keepdims=True)
        for k in range(8)
    ]
    w = w_ref[...]
    hi = w.astype(BF16)
    a_ref[0:TOK, :] = tok_ref[:, 0:PART]
    b_ref[...] = tok_ref[:, PART : 2 * PART]
    a_ref[TOK : TOK + 8, 0:128] = ids.astype(F32).astype(BF16)
    a_ref[TOK : TOK + 8, 128:256] = jnp.concatenate(ranks, axis=0).astype(BF16)
    a_ref[TOK : TOK + 8, 256:384] = hi
    a_ref[TOK : TOK + 8, 384:512] = (w - hi.astype(F32)).astype(BF16)


def slot_table(info, first, half, slots, values):
    ids = info[:, 0:128].astype(F32)
    rank = info[:, 128:256].astype(F32)
    mine = iota((PLANE, TOK), 0).astype(F32) + first.astype(F32)
    slot = jnp.full((PLANE, TOK), -1000.0, F32)
    picked = [jnp.zeros((PLANE, TOK), F32) for _ in values]
    for k in range(8):
        hit = ids[k : k + 1, :] == mine
        slot = jnp.where(hit, rank[k : k + 1, :], slot)
        for i, at in enumerate(values):
            value = info[:, at : at + 128].astype(F32)
            picked[i] = jnp.where(hit, value[k : k + 1, :], picked[i])
    slot = slot.astype(jnp.int32)
    if slots < CAP:
        slot = slot - half * slots
        slot = jnp.where((slot >= 0) & (slot < slots), slot, -1000)
    return slot, picked


def placed(row, value=None):
    hit = row[:, None, :] == iota((PLANE, SUB, TOK), 1)
    out = jnp.where(hit, 1.0 if value is None else value[:, None, :], 0.0)
    return out.astype(BF16).reshape(PLANE * SUB, TOK)


def dispatch_body(chunk, scal_ref, *refs):
    number = len(chunk)
    out_ref = refs[4 * number]
    tiles, left, first = plan(chunk)
    slots = {}
    for i, d in enumerate(chunk):
        info = refs[4 * i][TOK : TOK + 8, :]
        refs[4 * number + 1 + i][...] = info
        slot, _ = slot_table(info, scal_ref[0], scal_ref[1], PIECES[d], ())
        slots[d] = slot + first[d]
    for j in range(tiles):
        users = [(i, d) for i, d in enumerate(chunk) if j in tiles_of(chunk, d)[0]]
        onehot = jnp.concatenate([placed(slots[d] - SUB * j) for _, d in users], axis=1)
        for p in range(4):
            rows = jnp.concatenate([refs[4 * i + p][0:TOK, :] for i, _ in users], axis=0)
            at = j * WIDE + p * PART
            out_ref[:, at : at + PART] = jnp.dot(onehot, rows, preferred_element_type=F32).astype(BF16)
    if left:
        i = number - 1
        here = slots[chunk[i]] == tiles * SUB
        onehot = jnp.concatenate([placed(jnp.where(here, q, -1)) for q in range(SUB)], axis=1)
        per = PART // LEFT
        rows = jnp.concatenate(
            [
                refs[4 * i + q // per][0:TOK, q % per * LEFT : (q % per + 1) * LEFT]
                for q in range(SUB)
            ],
            axis=0,
        )
        out_ref[:, tiles * WIDE :] = jnp.dot(onehot, rows, preferred_element_type=F32).astype(BF16)


def expert_body(chunk, scal_ref, x_ref, gm_ref, gp_ref, um_ref, up_ref, dm_ref, dp_ref, out_ref, wm, wp, wd, sems):
    half = scal_ref[1]
    side_width = WIDE // 2
    copies = []
    for side in range(2):
        at = pl.multiple_of((half if side == 0 else 1 - half) * side_width, side_width)
        here = pl.ds(at, side_width)
        to = pl.ds(side * side_width, side_width)
        for i, (src, dst, lane) in enumerate(((gm_ref, wm, 0), (um_ref, wm, FH), (gp_ref, wp, 0), (up_ref, wp, FH))):
            copies.append((i, src.at[here, :], dst.at[to, pl.ds(lane, FH)]))
        for i, (src, row) in enumerate(((dm_ref, 0), (dp_ref, FH))):
            copies.append((4 + i, src.at[:, here], wd.at[pl.ds(row, FH), to]))
    copies.sort(key=lambda c: c[0])
    copies = [pltpu.make_async_copy(src, dst, sems.at[n]) for n, (_, src, dst) in enumerate(copies)]
    for c in copies:
        c.start()
    tiles, left, _ = plan(chunk)
    blocks = [x_ref[:, j * WIDE : (j + 1) * WIDE] for j in range(tiles)]
    if left:
        rows = x_ref[:, tiles * WIDE :]
        apart = iota((PLANE, PLANE * SUB), 1) - SUB * iota((PLANE, PLANE * SUB), 0)
        blocks.append(
            jnp.concatenate(
                [
                    jnp.dot(
                        jnp.where(apart == q, 1.0, 0.0).astype(BF16), rows, preferred_element_type=F32
                    ).astype(BF16)
                    for q in range(SUB)
                ],
                axis=1,
            )
        )
    x = jnp.concatenate(blocks, axis=0)
    hidden = []
    for i, w in enumerate((wm, wp)):
        for c in copies[4 * i : 4 * i + 4]:
            c.wait()
        both = jnp.dot(x, w[...], preferred_element_type=F32)
        gate = both[:, :FH]
        hidden.append((gate / (1.0 + jnp.exp(-gate)) * both[:, FH:]).astype(BF16))
    for c in copies[8:]:
        c.wait()
    y = jnp.dot(jnp.concatenate(hidden, axis=1), wd[...], preferred_element_type=F32).astype(BF16)
    size = PLANE * SUB
    for j in range(tiles):
        out_ref[:, j * WIDE : (j + 1) * WIDE] = y[j * size : (j + 1) * size, :]
    if left:
        apart = iota((size, PLANE), 0) - SUB * iota((size, PLANE), 1)
        total = None
        for q in range(SUB):
            spread = jnp.where(apart == q, 1.0, 0.0).astype(BF16)
            part = jnp.dot(spread, y[tiles * size :, q * LEFT : (q + 1) * LEFT], preferred_element_type=F32)
            total = part if total is None else total + part
        out_ref[:, tiles * WIDE :] = total.astype(BF16)


def combine_body(chunk, d, has_received, last, scal_ref, info_ref, *refs):
    tiles, _, first = plan(chunk)
    used, over = tiles_of(chunk, d)
    slot, values = slot_table(info_ref[...], scal_ref[0], scal_ref[1], PIECES[d], (256, 384))
    slot = slot + first[d]
    weights = jnp.concatenate([placed(slot - SUB * j, value) for j in used for value in values], axis=0)
    rows = jnp.concatenate([refs[n][...] for n in range(len(used)) for _ in values], axis=0)
    total = lax.dot_general(weights, rows, (((0,), (0,)), ((), ())), preferred_element_type=F32)
    at = len(used)
    if over:
        here = slot == tiles * SUB
        weights = jnp.concatenate(
            [
                jnp.concatenate([placed(jnp.where(here, q, -1), value) for q in range(SUB)], axis=1)
                for value in values
            ],
            axis=0,
        )
        rows = jnp.concatenate([refs[at][...] for _ in values], axis=0)
        extra = lax.dot_general(weights, rows, (((0,), (0,)), ((), ())), preferred_element_type=F32)
        total = total + jnp.concatenate([extra[q * TOK : (q + 1) * TOK, :] for q in range(SUB)], axis=1)
        at += 1
    parts = [total[:, p * PART : (p + 1) * PART] for p in range(4)]
    if has_received:
        parts = [part + refs[at + p][...].astype(F32) for p, part in enumerate(parts)]
        at += 4
    if last:
        for side in range(2):
            out = refs[at + side]
            out[...] = jnp.concatenate(parts[2 * side : 2 * side + 2], axis=1).astype(out.dtype)
    else:
        for p in range(4):
            refs[at + p][...] = parts[p].astype(BF16)


def whole(shape):
    return pl.BlockSpec(shape, lambda i: (0,) * len(shape))


def lane_block(shape, at):
    return pl.BlockSpec(shape, lambda i: (0, at))


SMEM = pl.BlockSpec(memory_space=pltpu.SMEM)
HBM = pl.BlockSpec(memory_space=pltpu.HBM)


def kernel(body, out, in_specs, scratch=(), vmem=16):
    return pl.pallas_call(
        body,
        out_shape=[jax.ShapeDtypeStruct(*o) for o in out],
        grid=(1,),
        in_specs=in_specs,
        out_specs=[whole(o[0]) for o in out],
        scratch_shapes=list(scratch),
        compiler_params=pltpu.CompilerParams(vmem_limit_bytes=vmem * 1024 * 1024),
    )


def staged(tokens, gate_weights, expert_ids, w_gate, w_up, w_down):
    z = lax.axis_index("z")
    half = lax.axis_index("half")
    zs = lax.axis_size("z")
    scal = jnp.stack([z * PLANE, half]).astype(jnp.int32)
    swap = [(0, 1), (1, 0)]
    forth = []
    for i in range(zs):
        forth.append((i * 2, (i + 1) % zs * 2))
        forth.append((i * 2 + 1, (i - 1) % zs * 2 + 1))
    back = [(b, a) for a, b in forth]
    size = PLANE * SUB

    shapes = ((TOK + 8, PART), (TOK, PART))
    own = kernel(
        route_body, [(s, BF16) for s in shapes], [whole((TOK, WIDE // 2)), whole((8, TOK)), whole((8, TOK))]
    )(tokens, expert_ids.T, gate_weights.T)
    other = [lax.ppermute(v, "half", swap) for v in own]
    held = {0: list(own) + other}
    for d in range(1, 5):
        held[d] = [lax.ppermute(v, ("z", "half"), forth) for v in held[d - 1]]
    mine = (w_gate[0], w_up[0], w_down[0])
    gated = lax.optimization_barrier((other[1],) + mine)
    theirs = [lax.ppermute(w, "half", swap) for w in gated[1:]]

    answers = {}
    for chunk in CHUNKS:
        lanes = lanes_of(chunk)
        arrays = [v for d in chunk for v in held[d]]
        sent, *infos = kernel(
            functools.partial(dispatch_body, chunk),
            [((size, lanes), BF16)] + [((8, PART), BF16) for _ in chunk],
            [SMEM] + [whole(v.shape) for v in arrays],
        )(scal, *arrays)
        got = lax.all_to_all(sent.reshape(PLANE, SUB, lanes), ("x", "y"), 0, 0, tiled=True)
        (result,) = kernel(
            functools.partial(expert_body, chunk),
            [((size, lanes), BF16)],
            [SMEM, whole((size, lanes))] + [HBM] * 6,
            (
                pltpu.VMEM((WIDE, 2 * FH), BF16),
                pltpu.VMEM((WIDE, 2 * FH), BF16),
                pltpu.VMEM((2 * FH, WIDE), BF16),
                pltpu.SemaphoreType.DMA((12,)),
            ),
            58,
        )(scal, got.reshape(size, lanes), mine[0], theirs[0], mine[1], theirs[1], mine[2], theirs[2])
        returned = lax.all_to_all(result.reshape(PLANE, SUB, lanes), ("x", "y"), 0, 0, tiled=True)
        for d, info in zip(chunk, infos):
            answers[d] = (chunk, returned.reshape(size, lanes), info)

    received = []
    for d in (4, 3, 2, 1, 0):
        chunk, value, info = answers[d]
        used, over = tiles_of(chunk, d)
        specs = [lane_block((size, WIDE), j) for j in used]
        if over:
            specs.append(lane_block((size, LEFT), plan(chunk)[0] * SUB))
        last = d == 0
        outs = kernel(
            functools.partial(combine_body, chunk, d, bool(received), last),
            [((TOK, 2 * PART), F32), ((TOK, 2 * PART), BF16)] if last else [((TOK, PART), BF16)] * 4,
            [SMEM, whole((8, PART))] + specs + [whole((TOK, PART)) for _ in received],
        )(scal, info, *[value for _ in specs], *received)
        if not last:
            received = [lax.ppermute(v, ("z", "half"), back) for v in outs]
    kept, given = outs
    return (kept + lax.ppermute(given, "half", swap).astype(F32)).astype(BF16)


def solution(mesh):
    spaced = Mesh(mesh.devices.reshape(8, 4, 4, 2), ("z", "x", "y", "half"))
    ep = ("z", "x", "y")
    specs = (
        P(ep, "half"),
        P(ep, None),
        P(ep, None),
        P(ep, None, "half"),
        P(ep, None, "half"),
        P(ep, "half", None),
    )
    return jax.shard_map(staged, mesh=spaced, in_specs=specs, out_specs=P(ep, "half"), check_vma=False)
```

```python
import functools

import jax
import jax.numpy as jnp
from jax import lax
from jax.experimental import pallas as pl
from jax.experimental.pallas import tpu as pltpu
from jax.sharding import Mesh, PartitionSpec as P


F32 = jnp.float32
BF16 = jnp.bfloat16
CAP = 10
TOK = 128
WIDE = 2048
HALF = 1024
PART = 512
FH = 384
PLANE = 16
SUB = 8
LEFT = WIDE // SUB
PIECES = {0: 5, 1: 10, 2: 10, 3: 10, 4: 5}
CHUNKS = ((0, 1, 2), (3, 4))
EXPERT_VMEM = 56
ROUTE_VMEM = 58


def iota(shape, dim):
    return lax.broadcasted_iota(jnp.int32, shape, dim)


def plan(chunk):
    first = {}
    n = 0
    for d in chunk:
        first[d] = n
        n += PIECES[d]
    left = n % SUB == 1
    tiles = n // SUB if left else -(-n // SUB)
    return tiles, left, first


def lanes_of(chunk):
    tiles, left, _ = plan(chunk)
    return tiles * WIDE + (LEFT if left else 0)


def tiles_of(chunk, d):
    tiles, left, first = plan(chunk)
    at, end = first[d], first[d] + PIECES[d]
    return [j for j in range(tiles) if at < (j + 1) * SUB and end > j * SUB], left and end > tiles * SUB


def route_body(tok_ref, ids_ref, w_ref, a_ref):
    ids = ids_ref[...]
    experts = iota((128, TOK), 0)
    named = jnp.zeros((128, TOK), F32)
    for k in range(8):
        named = jnp.where(ids[k : k + 1, :] == experts, 1.0, named)
    before = jnp.where(iota((TOK, TOK), 0) < iota((TOK, TOK), 1), 1.0, 0.0)
    count = jnp.dot(named.astype(BF16), before.astype(BF16), preferred_element_type=F32)
    ranks = [
        jnp.sum(jnp.where(ids[k : k + 1, :] == experts, count, 0.0), axis=0, keepdims=True)
        for k in range(8)
    ]
    w = w_ref[...]
    hi = w.astype(BF16)
    a_ref[0:TOK, :] = tok_ref[...]
    a_ref[TOK : TOK + 8, 0:128] = ids.astype(F32).astype(BF16)
    a_ref[TOK : TOK + 8, 128:256] = jnp.concatenate(ranks, axis=0).astype(BF16)
    a_ref[TOK : TOK + 8, 256:384] = hi
    a_ref[TOK : TOK + 8, 384:512] = (w - hi.astype(F32)).astype(BF16)
    a_ref[TOK : TOK + 8, 512:1024] = jnp.zeros((8, 512), BF16)


def slot_table(info, first, half, slots, values):
    ids = info[:, 0:128].astype(F32)
    rank = info[:, 128:256].astype(F32)
    mine = iota((PLANE, TOK), 0).astype(F32) + first.astype(F32)
    slot = jnp.full((PLANE, TOK), -1000.0, F32)
    picked = [jnp.zeros((PLANE, TOK), F32) for _ in values]
    for k in range(8):
        hit = ids[k : k + 1, :] == mine
        slot = jnp.where(hit, rank[k : k + 1, :], slot)
        for i, at in enumerate(values):
            value = info[:, at : at + 128].astype(F32)
            picked[i] = jnp.where(hit, value[k : k + 1, :], picked[i])
    slot = slot.astype(jnp.int32)
    if slots < CAP:
        slot = slot - half * slots
        slot = jnp.where((slot >= 0) & (slot < slots), slot, -1000)
    return slot, picked


def placed(row, value=None):
    hit = row[:, None, :] == iota((PLANE, SUB, TOK), 1)
    out = jnp.where(hit, 1.0 if value is None else value[:, None, :], 0.0)
    return out.astype(BF16).reshape(PLANE * SUB, TOK)


def dispatch_body(chunk, scal_ref, *refs):
    number = len(chunk)
    out_ref = refs[2 * number]
    tiles, left, first = plan(chunk)
    slots = {}
    for i, d in enumerate(chunk):
        info = refs[2 * i][TOK : TOK + 8, 0:512]
        refs[2 * number + 1 + i][...] = info
        slot, _ = slot_table(info, scal_ref[0], scal_ref[1], PIECES[d], ())
        slots[d] = slot + first[d]
    for j in range(tiles):
        users = [(i, d) for i, d in enumerate(chunk) if j in tiles_of(chunk, d)[0]]
        onehot = jnp.concatenate([placed(slots[d] - SUB * j) for _, d in users], axis=1)
        for p in range(2):
            rows = jnp.concatenate([refs[2 * i + p][0:TOK, :] for i, _ in users], axis=0)
            at = j * WIDE + p * HALF
            out_ref[:, at : at + HALF] = jnp.dot(onehot, rows, preferred_element_type=F32).astype(BF16)
    if left:
        i = number - 1
        here = slots[chunk[i]] == tiles * SUB
        onehot = jnp.concatenate([placed(jnp.where(here, q, -1)) for q in range(SUB)], axis=1)
        per = HALF // LEFT
        rows = jnp.concatenate(
            [
                refs[2 * i + q // per][0:TOK, q % per * LEFT : (q % per + 1) * LEFT]
                for q in range(SUB)
            ],
            axis=0,
        )
        out_ref[:, tiles * WIDE :] = jnp.dot(onehot, rows, preferred_element_type=F32).astype(BF16)


def expert_body(chunk, scal_ref, x_ref, gm_ref, gp_ref, um_ref, up_ref, dm_ref, dp_ref, out_ref, wm, wp, wd, sems):
    half = scal_ref[1]
    side_width = WIDE // 2
    copies = []
    for side in range(2):
        at = pl.multiple_of((half if side == 0 else 1 - half) * side_width, side_width)
        here = pl.ds(at, side_width)
        to = pl.ds(side * side_width, side_width)
        for i, (src, dst, lane) in enumerate(((gm_ref, wm, 0), (um_ref, wm, FH), (gp_ref, wp, 0), (up_ref, wp, FH))):
            copies.append((i, src.at[here, :], dst.at[to, pl.ds(lane, FH)]))
        for i, (src, row) in enumerate(((dm_ref, 0), (dp_ref, FH))):
            copies.append((4 + i, src.at[:, here], wd.at[pl.ds(row, FH), to]))
    copies.sort(key=lambda c: c[0])
    copies = [pltpu.make_async_copy(src, dst, sems.at[n]) for n, (_, src, dst) in enumerate(copies)]
    for c in copies:
        c.start()
    tiles, left, _ = plan(chunk)
    blocks = [x_ref[:, j * WIDE : (j + 1) * WIDE] for j in range(tiles)]
    if left:
        rows = x_ref[:, tiles * WIDE :]
        apart = iota((PLANE, PLANE * SUB), 1) - SUB * iota((PLANE, PLANE * SUB), 0)
        blocks.append(
            jnp.concatenate(
                [
                    jnp.dot(
                        jnp.where(apart == q, 1.0, 0.0).astype(BF16), rows, preferred_element_type=F32
                    ).astype(BF16)
                    for q in range(SUB)
                ],
                axis=1,
            )
        )
    x = jnp.concatenate(blocks, axis=0)
    hidden = []
    for i, w in enumerate((wm, wp)):
        for c in copies[4 * i : 4 * i + 4]:
            c.wait()
        both = jnp.dot(x, w[...], preferred_element_type=F32)
        gate = both[:, :FH]
        hidden.append((gate / (1.0 + jnp.exp(-gate)) * both[:, FH:]).astype(BF16))
    for c in copies[8:]:
        c.wait()
    y = jnp.dot(jnp.concatenate(hidden, axis=1), wd[...], preferred_element_type=F32).astype(BF16)
    size = PLANE * SUB
    for j in range(tiles):
        out_ref[:, j * WIDE : (j + 1) * WIDE] = y[j * size : (j + 1) * size, :]
    if left:
        apart = iota((size, PLANE), 0) - SUB * iota((size, PLANE), 1)
        total = None
        for q in range(SUB):
            spread = jnp.where(apart == q, 1.0, 0.0).astype(BF16)
            part = jnp.dot(spread, y[tiles * size :, q * LEFT : (q + 1) * LEFT], preferred_element_type=F32)
            total = part if total is None else total + part
        out_ref[:, tiles * WIDE :] = total.astype(BF16)


def combine_body(chunk, d, last, scal_ref, info_ref, *refs):
    tiles, _, first = plan(chunk)
    used, over = tiles_of(chunk, d)
    slot, values = slot_table(info_ref[...], scal_ref[0], scal_ref[1], PIECES[d], (256, 384))
    slot = slot + first[d]
    weights = jnp.concatenate([placed(slot - SUB * j, value) for j in used for value in values], axis=0)
    rows = jnp.concatenate([refs[n][...] for n in range(len(used)) for _ in values], axis=0)
    total = lax.dot_general(weights, rows, (((0,), (0,)), ((), ())), preferred_element_type=F32)
    at = len(used)
    if over:
        here = slot == tiles * SUB
        weights = jnp.concatenate(
            [
                jnp.concatenate([placed(jnp.where(here, q, -1), value) for q in range(SUB)], axis=1)
                for value in values
            ],
            axis=0,
        )
        rows = jnp.concatenate([refs[at][...] for _ in values], axis=0)
        extra = lax.dot_general(weights, rows, (((0,), (0,)), ((), ())), preferred_element_type=F32)
        total = total + jnp.concatenate([extra[q * TOK : (q + 1) * TOK, :] for q in range(SUB)], axis=1)
        at += 1
    parts = [total[:, p * PART : (p + 1) * PART] for p in range(4)]
    if last:
        parts = [part + refs[at + p][...].astype(F32) for p, part in enumerate(parts)]
        for side in range(2):
            out = refs[at + 4 + side]
            out[...] = jnp.concatenate(parts[2 * side : 2 * side + 2], axis=1).astype(out.dtype)
    else:
        for p in range(4):
            out = refs[at + p]
            out[...] = parts[p].astype(out.dtype)


def whole(shape):
    return pl.BlockSpec(shape, lambda i: (0,) * len(shape))


def lane_block(shape, at):
    return pl.BlockSpec(shape, lambda i: (0, at))


SMEM = pl.BlockSpec(memory_space=pltpu.SMEM)
HBM = pl.BlockSpec(memory_space=pltpu.HBM)


def kernel(body, out, in_specs, scratch=(), vmem=16):
    return pl.pallas_call(
        body,
        out_shape=[jax.ShapeDtypeStruct(*o) for o in out],
        grid=(1,),
        in_specs=in_specs,
        out_specs=[whole(o[0]) for o in out],
        scratch_shapes=list(scratch),
        compiler_params=pltpu.CompilerParams(vmem_limit_bytes=vmem * 1024 * 1024),
    )


def staged(tokens, gate_weights, expert_ids, w_gate, w_up, w_down):
    z = lax.axis_index("z")
    half = lax.axis_index("half")
    zs = lax.axis_size("z")
    scal = jnp.stack([z * PLANE, half]).astype(jnp.int32)
    swap = [(0, 1), (1, 0)]
    forth = []
    for i in range(zs):
        forth.append((i * 2, (i + 1) % zs * 2))
        forth.append((i * 2 + 1, (i - 1) % zs * 2 + 1))
    back = [(b, a) for a, b in forth]
    size = PLANE * SUB

    side = (TOK, HALF)
    other = lax.ppermute(tokens, "half", swap)
    (own,) = kernel(
        route_body, [((TOK + 8, HALF), BF16)], [whole(side), whole((8, TOK)), whole((8, TOK))], vmem=ROUTE_VMEM
    )(tokens, expert_ids.T, gate_weights.T)
    held = {0: [own, other]}
    for d in range(1, 5):
        held[d] = [lax.ppermute(v, ("z", "half"), forth) for v in held[d - 1]]
    mine = (w_gate[0], w_up[0], w_down[0])
    gated = lax.optimization_barrier((other,) + mine)
    theirs = [lax.ppermute(w, "half", swap) for w in gated[1:]]

    answers = {}
    for chunk in CHUNKS:
        lanes = lanes_of(chunk)
        arrays = [v for d in chunk for v in held[d]]
        sent, *infos = kernel(
            functools.partial(dispatch_body, chunk),
            [((size, lanes), BF16)] + [((8, 512), BF16) for _ in chunk],
            [SMEM] + [whole(v.shape) for v in arrays],
        )(scal, *arrays)
        got = lax.all_to_all(sent.reshape(PLANE, SUB, lanes), ("x", "y"), 0, 0, tiled=True)
        (result,) = kernel(
            functools.partial(expert_body, chunk),
            [((size, lanes), BF16)],
            [SMEM, whole((size, lanes))] + [HBM] * 6,
            (
                pltpu.VMEM((WIDE, 2 * FH), BF16),
                pltpu.VMEM((WIDE, 2 * FH), BF16),
                pltpu.VMEM((2 * FH, WIDE), BF16),
                pltpu.SemaphoreType.DMA((12,)),
            ),
            EXPERT_VMEM,
        )(scal, got.reshape(size, lanes), mine[0], theirs[0], mine[1], theirs[1], mine[2], theirs[2])
        returned = lax.all_to_all(result.reshape(PLANE, SUB, lanes), ("x", "y"), 0, 0, tiled=True)
        for d, info in zip(chunk, infos):
            answers[d] = (chunk, returned.reshape(size, lanes), info)

    received = []
    for d in (4, 3, 2, 1, 0):
        chunk, value, info = answers[d]
        used, over = tiles_of(chunk, d)
        specs = [lane_block((size, WIDE), j) for j in used]
        if over:
            specs.append(lane_block((size, LEFT), plan(chunk)[0] * SUB))
        last = d == 0
        extra = received if last else []
        outs = kernel(
            functools.partial(combine_body, chunk, d, last),
            [(side, F32), (side, BF16)] if last else [((TOK, PART), F32 if received else BF16)] * 4,
            [SMEM, whole((8, 512))] + specs + [whole((TOK, PART)) for _ in extra],
        )(scal, info, *[value for _ in specs], *extra)
        if not last:
            if received:
                outs = [(v + r.astype(F32)).astype(BF16) for v, r in zip(outs, received)]
            received = [lax.ppermute(v, ("z", "half"), back) for v in outs]
    kept, given = outs
    return (kept + lax.ppermute(given, "half", swap).astype(F32)).astype(BF16)


def solution(mesh):
    spaced = Mesh(mesh.devices.reshape(8, 4, 4, 2), ("z", "x", "y", "half"))
    ep = ("z", "x", "y")
    specs = (
        P(ep, "half"),
        P(ep, None),
        P(ep, None),
        P(ep, None, "half"),
        P(ep, None, "half"),
        P(ep, "half", None),
    )
    return jax.shard_map(staged, mesh=spaced, in_specs=specs, out_specs=P(ep, "half"), check_vma=False)
```

```python
import functools

import jax
import jax.numpy as jnp
from jax import lax
from jax.experimental import pallas as pl
from jax.experimental.pallas import tpu as pltpu
from jax.sharding import Mesh, PartitionSpec as P


F32 = jnp.float32
BF16 = jnp.bfloat16
CAP = 10
TOK = 128
WIDE = 2048
HALF = 1024
PART = 512
FH = 384
PLANE = 16
SUB = 8
LEFT = WIDE // SUB
PIECES = {0: 5, 1: 10, 2: 10, 3: 10, 4: 5}
CHUNKS = ((0,), (1, 2), (3, 4))
TAKES = ((0, 1), (2,))
EXPERT_VMEM = 56
ROUTE_VMEM = 58


def iota(shape, dim):
    return lax.broadcasted_iota(jnp.int32, shape, dim)


def parts_of(d):
    return PIECES[d] // SUB * SUB, PIECES[d] % SUB


def lanes_of(d):
    tile, rest = parts_of(d)
    return tile // SUB * WIDE + rest * LEFT


def width_of(chunk):
    return sum(lanes_of(d) for d in chunk)


def route_body(tok_ref, ids_ref, w_ref, out_ref):
    ids = ids_ref[...]
    experts = iota((128, TOK), 0)
    named = jnp.zeros((128, TOK), F32)
    for k in range(8):
        named = jnp.where(ids[k : k + 1, :] == experts, 1.0, named)
    before = jnp.where(iota((TOK, TOK), 0) < iota((TOK, TOK), 1), 1.0, 0.0)
    count = jnp.dot(named.astype(BF16), before.astype(BF16), preferred_element_type=F32)
    ranks = [
        jnp.sum(jnp.where(ids[k : k + 1, :] == experts, count, 0.0), axis=0, keepdims=True)
        for k in range(8)
    ]
    w = w_ref[...]
    hi = w.astype(BF16)
    out_ref[0:TOK, :] = tok_ref[...]
    out_ref[TOK : TOK + 8, 0:128] = ids.astype(F32).astype(BF16)
    out_ref[TOK : TOK + 8, 128:256] = jnp.concatenate(ranks, axis=0).astype(BF16)
    out_ref[TOK : TOK + 8, 256:384] = hi
    out_ref[TOK : TOK + 8, 384:512] = (w - hi.astype(F32)).astype(BF16)
    out_ref[TOK : TOK + 8, 512:1024] = jnp.zeros((8, 512), BF16)


def slot_table(info, first, half, slots, values):
    ids = info[:, 0:128].astype(F32)
    rank = info[:, 128:256].astype(F32)
    mine = iota((PLANE, TOK), 0).astype(F32) + first.astype(F32)
    slot = jnp.full((PLANE, TOK), -1000.0, F32)
    picked = [jnp.zeros((PLANE, TOK), F32) for _ in values]
    for k in range(8):
        hit = ids[k : k + 1, :] == mine
        slot = jnp.where(hit, rank[k : k + 1, :], slot)
        for i, at in enumerate(values):
            value = info[:, at : at + 128].astype(F32)
            picked[i] = jnp.where(hit, value[k : k + 1, :], picked[i])
    slot = slot.astype(jnp.int32)
    if slots < CAP:
        slot = slot - half * slots
        slot = jnp.where((slot >= 0) & (slot < slots), slot, -1000)
    return slot, picked


def placed(slot, d, value=None):
    tile, rest = parts_of(d)
    one = 1.0 if value is None else value
    out = []
    if tile:
        hit = slot[:, None, :] == iota((PLANE, SUB, TOK), 1)
        three = one if value is None else value[:, None, :]
        out.append(jnp.where(hit, three, 0.0).astype(BF16).reshape(PLANE * SUB, TOK))
    for s in range(tile, tile + rest):
        out.append(jnp.where(slot == s, one, 0.0).astype(BF16))
    return jnp.concatenate(out, axis=0)


def swapped():
    row, column = iota((PLANE * SUB, PLANE * SUB), 0), iota((PLANE * SUB, PLANE * SUB), 1)
    return jnp.where(column == (row & (PLANE - 1)) * SUB + (row >> 4), 1.0, 0.0).astype(BF16)


def unswapped():
    row, column = iota((PLANE * SUB, PLANE * SUB), 0), iota((PLANE * SUB, PLANE * SUB), 1)
    return jnp.where(row == (column & (PLANE - 1)) * SUB + (column >> 4), 1.0, 0.0).astype(BF16)


def packed(rows, number):
    z = jnp.concatenate(
        [
            jnp.concatenate(
                [rows[s * PLANE : (s + 1) * PLANE, q * LEFT : (q + 1) * LEFT] for s in range(number)],
                axis=1,
            )
            for q in range(SUB)
        ],
        axis=0,
    )
    return jnp.dot(unswapped(), z, preferred_element_type=F32).astype(BF16)


def unpacked(rows, number):
    z = jnp.dot(swapped(), rows, preferred_element_type=F32).astype(BF16)
    return [
        jnp.concatenate(
            [z[q * PLANE : (q + 1) * PLANE, s * LEFT : (s + 1) * LEFT] for q in range(SUB)], axis=1
        )
        for s in range(number)
    ]


def dispatch_body(chunk, scal_ref, *refs):
    number = len(chunk)
    out_ref = refs[2 * number]
    at = 0
    for i, d in enumerate(chunk):
        a_ref, b_ref = refs[2 * i], refs[2 * i + 1]
        tile, rest = parts_of(d)
        info = a_ref[TOK : TOK + 8, 0:512]
        refs[2 * number + 1 + i][...] = info
        slot, _ = slot_table(info, scal_ref[0], scal_ref[1], PIECES[d], ())
        onehot = placed(slot, d)
        rows = jnp.concatenate(
            [
                jnp.dot(onehot, ref[0:TOK, :], preferred_element_type=F32).astype(BF16)
                for ref in (a_ref, b_ref)
            ],
            axis=1,
        )
        if tile:
            out_ref[:, at : at + WIDE] = rows[0 : PLANE * tile, :]
            at += WIDE
        out_ref[:, at : at + rest * LEFT] = packed(rows[PLANE * tile :, :], rest)
        at += rest * LEFT


def places(chunks):
    out = []
    for n, chunk in enumerate(chunks):
        at = 0
        for d in chunk:
            out.append((n, d, at))
            at += lanes_of(d)
    return out


def expert_body(chunks, scal_ref, *refs):
    number = len(chunks)
    xs = refs[:number]
    gm_ref, gp_ref, um_ref, up_ref, dm_ref, dp_ref = refs[number : number + 6]
    outs = refs[number + 6 : 2 * number + 6]
    wm, wp, wd, sems = refs[2 * number + 6 :]
    half = scal_ref[1]
    copies = []
    for side in range(2):
        at = pl.multiple_of((half if side == 0 else 1 - half) * HALF, HALF)
        here = pl.ds(at, HALF)
        to = pl.ds(side * HALF, HALF)
        for i, (src, dst, lane) in enumerate(((gm_ref, wm, 0), (um_ref, wm, FH), (gp_ref, wp, 0), (up_ref, wp, FH))):
            copies.append((i // 2 * 2 + side, src.at[here, :], dst.at[to, pl.ds(lane, FH)]))
        for src, row in ((dm_ref, 0), (dp_ref, FH)):
            copies.append((4, src.at[:, here], wd.at[pl.ds(row, FH), to]))
    copies.sort(key=lambda c: c[0])
    copies = [pltpu.make_async_copy(src, dst, sems.at[n]) for n, (_, src, dst) in enumerate(copies)]
    for c in copies:
        c.start()
    spots = places(chunks)
    blocks = [xs[n][:, at : at + WIDE] for n, d, at in spots if parts_of(d)[0]]
    for n, d, at in spots:
        tile, rest = parts_of(d)
        at += tile // SUB * WIDE
        blocks += unpacked(xs[n][:, at : at + rest * LEFT], rest)
    x = jnp.concatenate(blocks, axis=0)
    hidden = []
    for i, w in enumerate((wm, wp)):
        both = None
        for side in range(2):
            for c in copies[4 * i + 2 * side : 4 * i + 2 * side + 2]:
                c.wait()
            to = slice(side * HALF, (side + 1) * HALF)
            part = jnp.dot(x[:, to], w[to, :], preferred_element_type=F32)
            both = part if both is None else both + part
        gate = both[:, :FH]
        hidden.append((gate / (1.0 + jnp.exp(-gate)) * both[:, FH:]).astype(BF16))
    for c in copies[8:]:
        c.wait()
    y = jnp.dot(jnp.concatenate(hidden, axis=1), wd[...], preferred_element_type=F32).astype(BF16)
    size = PLANE * SUB
    row = 0
    for n, d, at in spots:
        if parts_of(d)[0]:
            outs[n][:, at : at + WIDE] = y[row : row + size, :]
            row += size
    for n, d, at in spots:
        tile, rest = parts_of(d)
        at += tile // SUB * WIDE
        outs[n][:, at : at + rest * LEFT] = packed(y[row : row + rest * PLANE, :], rest)
        row += rest * PLANE


def combine_body(d, last, scal_ref, info_ref, y_ref, *refs):
    tile, rest = parts_of(d)
    slot, values = slot_table(info_ref[...], scal_ref[0], scal_ref[1], PIECES[d], (256, 384))
    weights = jnp.concatenate([placed(slot, d, value) for value in values], axis=0)
    rows = [y_ref[:, 0:WIDE]] if tile else []
    rows += unpacked(y_ref[:, tile // SUB * WIDE :], rest)
    rows = jnp.concatenate(rows * 2, axis=0)
    total = lax.dot_general(weights, rows, (((0,), (0,)), ((), ())), preferred_element_type=F32)
    parts = [total[:, p * PART : (p + 1) * PART] for p in range(4)]
    if last:
        parts = [part + refs[p][...].astype(F32) for p, part in enumerate(parts)]
        for side in range(2):
            out = refs[4 + side]
            out[...] = jnp.concatenate(parts[2 * side : 2 * side + 2], axis=1).astype(out.dtype)
    else:
        for p in range(4):
            refs[p][...] = parts[p].astype(refs[p].dtype)


def whole(shape):
    return pl.BlockSpec(shape, lambda i: (0,) * len(shape))


def lane_block(shape, at):
    return pl.BlockSpec(shape, lambda i: (0, at))


SMEM = pl.BlockSpec(memory_space=pltpu.SMEM)
HBM = pl.BlockSpec(memory_space=pltpu.HBM)


def kernel(body, out, in_specs, scratch=(), vmem=16):
    return pl.pallas_call(
        body,
        out_shape=[jax.ShapeDtypeStruct(*o) for o in out],
        grid=(1,),
        in_specs=in_specs,
        out_specs=[whole(o[0]) for o in out],
        scratch_shapes=list(scratch),
        compiler_params=pltpu.CompilerParams(vmem_limit_bytes=vmem * 1024 * 1024),
    )


def staged(tokens, gate_weights, expert_ids, w_gate, w_up, w_down):
    z = lax.axis_index("z")
    half = lax.axis_index("half")
    zs = lax.axis_size("z")
    scal = jnp.stack([z * PLANE, half]).astype(jnp.int32)
    swap = [(0, 1), (1, 0)]
    forth = []
    for i in range(zs):
        forth.append((i * 2, (i + 1) % zs * 2))
        forth.append((i * 2 + 1, (i - 1) % zs * 2 + 1))
    back = [(b, a) for a, b in forth]
    size = PLANE * SUB

    side = (TOK, HALF)
    other = lax.ppermute(tokens, "half", swap)
    (own,) = kernel(
        route_body,
        [((TOK + 8, HALF), BF16)],
        [whole(side), whole((8, TOK)), whole((8, TOK))],
        vmem=ROUTE_VMEM,
    )(tokens, expert_ids.T, gate_weights.T)
    held = {0: [own, other]}
    for d in range(1, 5):
        held[d] = [lax.ppermute(v, ("z", "half"), forth) for v in held[d - 1]]
    mine = (w_gate[0], w_up[0], w_down[0])
    gated = lax.optimization_barrier((other,) + mine)
    theirs = [lax.ppermute(w, "half", swap) for w in gated[1:]]

    infos = {}
    gots = []
    for chunk in CHUNKS:
        width = width_of(chunk)
        arrays = [v for d in chunk for v in held[d]]
        sent, *seen = kernel(
            functools.partial(dispatch_body, chunk),
            [((size, width), BF16)] + [((8, 512), BF16) for _ in chunk],
            [SMEM] + [whole(v.shape) for v in arrays],
        )(scal, *arrays)
        infos.update(zip(chunk, seen))
        got = lax.all_to_all(sent.reshape(PLANE, SUB, width), ("x", "y"), 0, 0, tiled=True)
        gots.append(got.reshape(size, width))
    results = {}
    for takes in TAKES:
        arrays = [gots[n] for n in takes]
        made = kernel(
            functools.partial(expert_body, [CHUNKS[n] for n in takes]),
            [(v.shape, BF16) for v in arrays],
            [SMEM] + [whole(v.shape) for v in arrays] + [HBM] * 6,
            (
                pltpu.VMEM((WIDE, 2 * FH), BF16),
                pltpu.VMEM((WIDE, 2 * FH), BF16),
                pltpu.VMEM((2 * FH, WIDE), BF16),
                pltpu.SemaphoreType.DMA((12,)),
            ),
            EXPERT_VMEM,
        )(scal, *arrays, mine[0], theirs[0], mine[1], theirs[1], mine[2], theirs[2])
        results.update(zip(takes, made))

    received = []
    for n in (2, 1, 0):
        chunk = CHUNKS[n]
        width = width_of(chunk)
        value = lax.all_to_all(results[n].reshape(PLANE, SUB, width), ("x", "y"), 0, 0, tiled=True)
        value = value.reshape(size, width)
        for d in reversed(chunk):
            lanes = lanes_of(d)
            at = sum(lanes_of(e) for e in chunk if e < d)
            last = d == 0
            extra = received if last else []
            outs = kernel(
                functools.partial(combine_body, d, last),
                [(side, F32), (side, BF16)] if last else [((TOK, PART), F32 if received else BF16)] * 4,
                [SMEM, whole((8, 512)), lane_block((size, lanes), at // lanes)]
                + [whole((TOK, PART)) for _ in extra],
            )(scal, infos[d], value, *extra)
            if not last:
                if received:
                    outs = [(v + r.astype(F32)).astype(BF16) for v, r in zip(outs, received)]
                received = [lax.ppermute(v, ("z", "half"), back) for v in outs]
    kept, given = outs
    return (kept + lax.ppermute(given, "half", swap).astype(F32)).astype(BF16)


def solution(mesh):
    spaced = Mesh(mesh.devices.reshape(8, 4, 4, 2), ("z", "x", "y", "half"))
    ep = ("z", "x", "y")
    specs = (
        P(ep, "half"),
        P(ep, None),
        P(ep, None),
        P(ep, None, "half"),
        P(ep, None, "half"),
        P(ep, "half", None),
    )
    return jax.shard_map(
        staged, mesh=spaced, in_specs=specs, out_specs=P(ep, "half"), check_vma=False
    )
```
